32 devices in a mesh: row: 4 (over z), col: 4 (over x, core), layer: 2 (over y).
Axes of the slice: x: 2, y: 2, z: 4, core: 2. Of those that a mesh axis runs over, the one named last changes fastest.
Arguments:
- left: bfloat16 [4096, 8192], P('row', ('col', 'layer')), may hold values from -6 to 6
- middle: bfloat16 [8192, 8192], P('row', 'col'), may hold values from -0.0625 to 0.0625
- right: bfloat16 [8192, 8192], P('row', 'col'), may hold values from -0.0625 to 0.0625
Outputs:
- product: bfloat16 [4096, 8192], P('row', ('col', 'layer'))
The draws below stay inside these ranges and needn't reach their ends.
All inputs are finite; a program needn't handle non-finite values.
Results may differ from the reference program's by a relative error of at most 0.0049.
Values may be sent and summed in bfloat16 or wider, within the bound.
No kernel may reach another device: no remote copies, remote signals or barrier semaphores. Data moves between devices by JAX's collectives and lax.ppermute only.
A program may use at most 128 MiB of HBM per device.

```python
import jax
import jax.numpy as jnp

K = 8192
N = 8192
P_SIZE = 8192
M = 4096


def block_scale(rng, dims, pieces, low, high):
    loudness, own = 1.0, jax.random.fold_in(rng, 6)
    for axis_at, shards_of in pieces:
        heights = jnp.exp(jax.random.uniform(jax.random.fold_in(own, axis_at), (shards_of,), jnp.float32, low / len(pieces), high / len(pieces)))
        loudness = loudness * jnp.repeat(heights, dims[axis_at] // shards_of).reshape([-1 if axis == axis_at else 1 for axis in range(len(dims))])
    return loudness


def scatter_about(key, dims, deviation, limit, shards=(), kind=jnp.bfloat16):
    array = jax.random.normal(key, dims, jnp.float32) * deviation
    if len(shards) > 0:
        array = block_scale(key, dims, shards, -0.22, 0.18) * array
    return jnp.clip(array, min=-limit, max=limit).astype(kind)


def setup_inputs(seed: int = 0) -> dict:
    streams_of = jax.random.split(jax.random.key(seed), 4)
    return {
        "left": scatter_about(streams_of[0], (M, K), 1.0, 6.0, ((0, 4), (1, 8))),
        "middle": scatter_about(streams_of[1], (K, N), K ** -0.5, 0.0625, ((0, 4), (1, 4))),
        "right": scatter_about(streams_of[2], (N, P_SIZE), N ** -0.5, 0.0625, ((0, 4), (1, 4))),
    }


def reference(left, middle, right):
    first = jnp.dot(left, middle, preferred_element_type=jnp.float32).astype(jnp.bfloat16)
    return jnp.dot(first, right, preferred_element_type=jnp.float32).astype(jnp.bfloat16)
```

```python
import jax
import jax.numpy as jnp
from jax import lax
from jax.sharding import PartitionSpec as P

AXES = ("row", "col", "layer")
PIECES = 4


def general(left, middle, right):
    def multiply(a, b):
        width = a.shape[1]
        layers = lax.axis_size("layer")
        groups = b.shape[0] // width // layers
        shaped = b.reshape(groups, layers, width, b.shape[1])
        own = lax.dynamic_index_in_dim(shaped, lax.axis_index("layer"), 1, keepdims=False)
        rows = lax.all_gather(own.reshape(groups * width, b.shape[1]), "row", axis=0, tiled=True)
        return jnp.dot(lax.all_gather(a, "col", axis=1, tiled=True), rows, preferred_element_type=jnp.float32)

    partial_value = multiply(left, middle)
    total = lax.psum(partial_value, "layer")
    half = partial_value.shape[1] // lax.axis_size("layer")
    first = lax.dynamic_slice_in_dim(total, lax.axis_index("layer") * half, half, 1).astype(jnp.bfloat16)
    second = multiply(first, right)
    return lax.psum_scatter(second, "layer", scatter_dimension=1, tiled=True).astype(jnp.bfloat16)


def stationary(left, middle, right):
    rows, cols, layers = (lax.axis_size(a) for a in AXES)
    r, c, l = (lax.axis_index(a) for a in AXES)

    def send(x, to):
        pairs = []
        for i in range(rows):
            for j in range(cols):
                for k in range(layers):
                    t = to(i, j, k)
                    if t is not None:
                        pairs.append(((i * cols + j) * layers + k, (t[0] * cols + t[1]) * layers + t[2]))
        return lax.ppermute(x, AXES, pairs)

    def keeps(i, j):
        return i ^ j in (0, 3)

    def home(i, j):
        return (i ^ j) & 1 == 0

    across_layer = lambda x: send(x, lambda i, j, k: (i, j, 1 - k))
    to_keeper = lambda x: send(x, lambda i, j, k: None if keeps(i, j) else (i ^ 1, j, k))
    keepers_swap = lambda x: send(x, lambda i, j, k: (i ^ 3, j, k) if keeps(i, j) else None)
    over_x = lambda x: send(x, lambda i, j, k: (i, j ^ 2, k) if keeps(i, j) else None)
    to_home = lambda x: send(x, lambda i, j, k: None if home(i, j) else (i ^ 3, j, k))
    over_core = lambda x: send(x, lambda i, j, k: (i, j ^ 1, k) if home(i, j) else None)
    near = lambda x: send(x, lambda i, j, k: (i ^ 1, j, k))
    far = lambda x: send(x, lambda i, j, k: (i ^ 3, j, k))

    is_keeper = ((r ^ c) == 0) | ((r ^ c) == 3)
    is_home = ((r ^ c) & 1) == 0
    f32 = lambda x: x.astype(jnp.float32)
    bf16 = lambda x: x.astype(jnp.bfloat16)

    def spread(pair):
        held = jnp.where(is_keeper, pair, over_x(pair))
        full = jnp.concatenate([held, to_home(held)], axis=0)
        return jnp.where(is_home, full, over_core(full))

    def times(a, w):
        return bf16(jnp.dot(a, w, preferred_element_type=jnp.float32))

    half = left.shape[0] // layers
    width = left.shape[1]
    b = half // PIECES
    mine = lax.dynamic_slice_in_dim(left, l * half, half, 0)
    theirs = lax.dynamic_slice_in_dim(left, (1 - l) * half, half, 0)
    own_parts, other_parts = [], []
    for p in range(PIECES):
        keep = mine[p * b : (p + 1) * b]
        got = across_layer(theirs[p * b : (p + 1) * b])
        x = jnp.where(l == 0, jnp.concatenate([keep, got], axis=1), jnp.concatenate([got, keep], axis=1))
        a = spread(jnp.concatenate([x, to_keeper(x)], axis=0))

        part = times(a, middle)
        n = part.shape[1]
        part = part.reshape(2, 2, b, n)
        got = to_keeper(part)[:, ::-1]
        got_far = keepers_swap(bf16(f32(part[1]) + f32(got[1])))
        first = bf16(f32(part[0]) + f32(got[0]) + f32(got_far)).reshape(2 * b, n)
        a = spread(first)

        part = times(a, right)
        n = part.shape[1]
        part = part.reshape(2, 2, b, n)
        if p % 4 != 3:
            got = near(part[:, 1])
            got_far = far(bf16(f32(part[1, 0]) + f32(got[1])))
            out = bf16(f32(part[0, 0]) + f32(got[0]) + f32(got_far))
        else:
            got = far(part[1])
            got_near = near(bf16(f32(part[0, 1]) + f32(got[1])))
            out = bf16(f32(part[0, 0]) + f32(got[0]) + f32(got_near))
        own_parts.append(lax.dynamic_slice_in_dim(out, l * width, width, 1))
        other_parts.append(across_layer(lax.dynamic_slice_in_dim(out, (1 - l) * width, width, 1)))
    own = jnp.concatenate(own_parts, axis=0)
    other = jnp.concatenate(other_parts, axis=0)
    return jnp.where(l == 0, jnp.concatenate([own, other], axis=0), jnp.concatenate([other, own], axis=0))


def solution(mesh):
    shape = mesh.shape
    fits = shape["row"] == shape["col"] == 4 and shape["layer"] == 2
    return jax.shard_map(
        stationary if fits else general,
        mesh=mesh,
        in_specs=(P("row", ("col", "layer")), P("row", "col"), P("row", "col")),
        out_specs=P("row", ("col", "layer")),
        check_vma=False,
    )
```

```python
import jax
import jax.numpy as jnp
from jax import lax
from jax.sharding import PartitionSpec as P

AXES = ("row", "col", "layer")
PIECES = 2
STRIPS = 2


def general(left, middle, right):
    def multiply(a, b):
        width = a.shape[1]
        layers = lax.axis_size("layer")
        groups = b.shape[0] // width // layers
        shaped = b.reshape(groups, layers, width, b.shape[1])
        own = lax.dynamic_index_in_dim(shaped, lax.axis_index("layer"), 1, keepdims=False)
        rows = lax.all_gather(own.reshape(groups * width, b.shape[1]), "row", axis=0, tiled=True)
        return jnp.dot(lax.all_gather(a, "col", axis=1, tiled=True), rows, preferred_element_type=jnp.float32)

    partial_value = multiply(left, middle)
    total = lax.psum(partial_value, "layer")
    half = partial_value.shape[1] // lax.axis_size("layer")
    first = lax.dynamic_slice_in_dim(total, lax.axis_index("layer") * half, half, 1).astype(jnp.bfloat16)
    second = multiply(first, right)
    return lax.psum_scatter(second, "layer", scatter_dimension=1, tiled=True).astype(jnp.bfloat16)


def inner_planes(left, middle, right):
    rows, cols, layers = (lax.axis_size(a) for a in AXES)
    r, c, l = (lax.axis_index(a) for a in AXES)
    side, x, core = r >> 1, c >> 1, c & 1

    def send(v, to):
        pairs = []
        for i in range(rows):
            for j in range(cols):
                for k in range(layers):
                    t = to(i, j, k)
                    if t is not None:
                        pairs.append(((i * cols + j) * layers + k, (t[0] * cols + t[1]) * layers + t[2]))
        return lax.ppermute(v, AXES, pairs)

    inner = lambda i: i in (1, 2)
    inwards = lambda v: send(v, lambda i, j, k: None if inner(i) else (i ^ 1, j, k))
    outwards = lambda v: send(v, lambda i, j, k: (i ^ 1, j, k) if inner(i) else None)
    across = lambda v: send(v, lambda i, j, k: (i ^ 3, j, k) if inner(i) else None)
    over_x = lambda v: send(v, lambda i, j, k: (i, j ^ 2, k) if inner(i) else None)
    over_core = lambda v: send(v, lambda i, j, k: (i, j ^ 1, k) if inner(i) else None)
    inner_layers = lambda v: send(v, lambda i, j, k: (i, j, 1 - k) if inner(i) else None)
    over_layer = lambda v: send(v, lambda i, j, k: (i, j, 1 - k))

    is_inner = (r == 1) | (r == 2)
    straight = x == side
    own_first = core == (r & 1)
    f32 = lambda v: v.astype(jnp.float32)
    bf16 = lambda v: v.astype(jnp.bfloat16)

    def in_order(flag, a, b, axis):
        return jnp.where(flag, jnp.concatenate([a, b], axis), jnp.concatenate([b, a], axis))

    def neighbour_weights(w):
        part = w.shape[0] // layers
        got = inwards(lax.dynamic_slice_in_dim(w, l * part, part, 0))
        return in_order(l == 0, got, inner_layers(got), 0)

    def times(a, b, own, outer):
        for_own, for_outer = jnp.where(own_first, a, b), jnp.where(own_first, b, a)
        dot = lambda u, v: jnp.dot(u, v, preferred_element_type=jnp.float32)
        return bf16(dot(for_own, own) + dot(for_outer, outer))

    half = left.shape[0] // layers
    width = left.shape[1]
    b = half // PIECES
    n = middle.shape[1]
    s = n // STRIPS
    mine = lax.dynamic_slice_in_dim(left, l * half, half, 0)
    theirs = lax.dynamic_slice_in_dim(left, (1 - l) * half, half, 0)

    def operand(p):
        keep = mine[p * b : (p + 1) * b]
        got = over_layer(theirs[p * b : (p + 1) * b])
        block = in_order(l == 0, keep, got, 1)
        pair = jnp.concatenate([block, inwards(block)], axis=0)
        other = over_x(pair)
        stay, go = jnp.where(straight, pair, other), jnp.where(straight, other, pair)
        a = jnp.concatenate([stay, across(go)], axis=0)
        return a, over_core(a)

    def reduce_first(part):
        part = part.reshape(4, 2, b // 2, part.shape[1])
        other = over_x(part[:, 1])
        stay, go = jnp.where(straight, part[:, 0], other), jnp.where(straight, other, part[:, 0])
        got = across(go)
        got = jnp.concatenate([got[2:], got[:2]], axis=0)
        done = bf16(f32(stay) + f32(got))
        a = jnp.stack([done, over_x(done)]).reshape(4 * b, part.shape[3])
        return a, over_core(a)

    def reduce_second(part):
        part = part.reshape(2, 2, 2, b // 2, part.shape[1])
        got = across(part[:, 1])
        total = bf16(f32(part[:, 0]) + f32(got[::-1]))
        final = jnp.where(is_inner, total[:, 0], outwards(total[:, 1]))
        keep = lax.dynamic_slice_in_dim(final, l * width, width, 2)
        got = over_layer(lax.dynamic_slice_in_dim(final, (1 - l) * width, width, 2))
        return keep, got

    strips = [(middle[:, i * s : (i + 1) * s], neighbour_weights(middle[:, i * s : (i + 1) * s])) for i in range(STRIPS)]
    operands = [operand(p) for p in range(PIECES)]
    right_outer = neighbour_weights(right)
    firsts = [[reduce_first(times(*operands[p], *strips[i])) for i in range(STRIPS)] for p in range(PIECES)]
    results = []
    for p in range(PIECES):
        a = jnp.concatenate([firsts[p][i][0] for i in range(STRIPS)], axis=1)
        o = jnp.concatenate([firsts[p][i][1] for i in range(STRIPS)], axis=1)
        results.append(reduce_second(times(a, o, right, right_outer)))
    order = lambda v: jnp.where(straight, v, v[::-1]).reshape(b, width)
    own = jnp.concatenate([order(k) for k, _ in results], axis=0)
    other = jnp.concatenate([order(g) for _, g in results], axis=0)
    return in_order(l == 0, own, other, 0)


def solution(mesh):
    shape = mesh.shape
    fits = shape["row"] == shape["col"] == 4 and shape["layer"] == 2
    return jax.shard_map(
        inner_planes if fits else general,
        mesh=mesh,
        in_specs=(P("row", ("col", "layer")), P("row", "col"), P("row", "col")),
        out_specs=P("row", ("col", "layer")),
        check_vma=False,
    )
```

```python
import jax
import jax.numpy as jnp
from jax import lax
from jax.sharding import PartitionSpec as P

AXES = ("row", "col", "layer")
PIECES = 2
STRIPS = 2


def general(left, middle, right):
    def multiply(a, b):
        width = a.shape[1]
        layers = lax.axis_size("layer")
        groups = b.shape[0] // width // layers
        shaped = b.reshape(groups, layers, width, b.shape[1])
        own = lax.dynamic_index_in_dim(shaped, lax.axis_index("layer"), 1, keepdims=False)
        rows = lax.all_gather(own.reshape(groups * width, b.shape[1]), "row", axis=0, tiled=True)
        return jnp.dot(lax.all_gather(a, "col", axis=1, tiled=True), rows, preferred_element_type=jnp.float32)

    partial_value = multiply(left, middle)
    total = lax.psum(partial_value, "layer")
    half = partial_value.shape[1] // lax.axis_size("layer")
    first = lax.dynamic_slice_in_dim(total, lax.axis_index("layer") * half, half, 1).astype(jnp.bfloat16)
    second = multiply(first, right)
    return lax.psum_scatter(second, "layer", scatter_dimension=1, tiled=True).astype(jnp.bfloat16)


def paired_rows(left, middle, right):
    rows, cols, layers = (lax.axis_size(a) for a in AXES)
    r, c, l = (lax.axis_index(a) for a in AXES)
    side, x, core = r >> 1, c >> 1, c & 1

    def send(v, name, to):
        pairs = []
        for i in range(rows):
            for j in range(cols):
                for k in range(layers):
                    t = to(i, j, k)
                    pairs.append(((i * cols + j) * layers + k, (t[0] * cols + t[1]) * layers + t[2]))
        with jax.named_scope(name):
            return lax.ppermute(v, AXES, pairs)

    beside = lambda v, name: send(v, name, lambda i, j, k: (i ^ 1, j, k))
    across = lambda v, name: send(v, name, lambda i, j, k: (i ^ 3, j, k))
    over_x = lambda v, name: send(v, name, lambda i, j, k: (i, j ^ 2, k))
    over_core = lambda v, name: send(v, name, lambda i, j, k: (i, j ^ 1, k))
    over_layer = lambda v, name: send(v, name, lambda i, j, k: (i, j, 1 - k))

    straight = x == side
    own_first = core == (r & 1)
    f32 = lambda v: v.astype(jnp.float32)
    bf16 = lambda v: v.astype(jnp.bfloat16)

    def in_order(flag, a, b, axis):
        return jnp.where(flag, jnp.concatenate([a, b], axis), jnp.concatenate([b, a], axis))

    def both_weights(w, name):
        part = w.shape[0] // layers
        got = beside(lax.dynamic_slice_in_dim(w, l * part, part, 0), name + "z")
        return jnp.concatenate([w, in_order(l == 0, got, over_layer(got, name + "y"), 0)], axis=0)

    def times(a, b, weights, name):
        with jax.named_scope(name):
            operand = in_order(own_first, a, b, 1)
            return bf16(jnp.dot(operand, weights, preferred_element_type=jnp.float32))

    half = left.shape[0] // layers
    width = left.shape[1]
    b = half // PIECES
    n = middle.shape[1]
    s = n // STRIPS
    mine = lax.dynamic_slice_in_dim(left, l * half, half, 0)
    theirs = lax.dynamic_slice_in_dim(left, (1 - l) * half, half, 0)

    def operand(p):
        keep = mine[p * b : (p + 1) * b]
        got = over_layer(theirs[p * b : (p + 1) * b], f"ty{p}")
        block = in_order(l == 0, keep, got, 1)
        other = over_x(block, f"tx{p}")
        stay, go = jnp.where(straight, block, other), jnp.where(straight, other, block)
        a = jnp.concatenate([stay, across(go, f"ta{p}")], axis=0)
        return a, over_core(a, f"tc{p}")

    def reduce_first(part, name):
        part = part.reshape(2, 2, b // 2, part.shape[1])
        other = over_x(part[:, 1], "fx" + name)
        stay, go = jnp.where(straight, part[:, 0], other), jnp.where(straight, other, part[:, 0])
        got = across(go, "fa" + name)
        done = bf16(f32(stay) + f32(got[::-1]))
        a = jnp.stack([done, over_x(done, "fg" + name)]).reshape(2 * b, part.shape[3])
        return a, over_core(a, "fc" + name)

    def reduce_second(part, p):
        part = part.reshape(2, 2, b // 2, part.shape[1])
        got = across(part[:, 1], f"sa{p}")
        final = bf16(f32(part[:, 0]) + f32(got[::-1]))
        keep = lax.dynamic_slice_in_dim(final, l * width, width, 2)
        return keep, over_layer(lax.dynamic_slice_in_dim(final, (1 - l) * width, width, 2), f"sy{p}")

    strips = [both_weights(middle[:, i * s : (i + 1) * s], f"m{i}") for i in range(STRIPS)]
    operands = [operand(p) for p in range(PIECES)]
    right_weights = both_weights(right, "r0")
    firsts = [[reduce_first(times(*operands[p], strips[i], f"m{p}_{i}"), f"{p}_{i}") for i in range(STRIPS)] for p in range(PIECES)]
    results = []
    for p in range(PIECES):
        a = jnp.concatenate([firsts[p][i][0] for i in range(STRIPS)], axis=1)
        o = jnp.concatenate([firsts[p][i][1] for i in range(STRIPS)], axis=1)
        results.append(reduce_second(times(a, o, right_weights, f"n{p}"), p))
    order = lambda v: jnp.where(straight, v, v[::-1]).reshape(b, width)
    own = jnp.concatenate([order(k) for k, _ in results], axis=0)
    other = jnp.concatenate([order(g) for _, g in results], axis=0)
    return in_order(l == 0, own, other, 0)


def solution(mesh):
    shape = mesh.shape
    fits = shape["row"] == shape["col"] == 4 and shape["layer"] == 2
    return jax.shard_map(
        paired_rows if fits else general,
        mesh=mesh,
        in_specs=(P("row", ("col", "layer")), P("row", "col"), P("row", "col")),
        out_specs=P("row", ("col", "layer")),
        check_vma=False,
    )
```

```python
import functools

import jax
import jax.numpy as jnp
from jax import lax
from jax.experimental import pallas as pl
from jax.experimental.pallas import tpu as pltpu
from jax.sharding import PartitionSpec as P


AXES = ("row", "col", "layer")
PIECES = 2
STRIPS = 2
FETCHES = {"m0": 2, "m1": 2, "r0": 2, "r1": 4}


def general(left, middle, right):
    def multiply(a, b):
        width = a.shape[1]
        layers = lax.axis_size("layer")
        groups = b.shape[0] // width // layers
        shaped = b.reshape(groups, layers, width, b.shape[1])
        own = lax.dynamic_index_in_dim(shaped, lax.axis_index("layer"), 1, keepdims=False)
        rows = lax.all_gather(own.reshape(groups * width, b.shape[1]), "row", axis=0, tiled=True)
        return jnp.dot(lax.all_gather(a, "col", axis=1, tiled=True), rows, preferred_element_type=jnp.float32)

    partial_value = multiply(left, middle)
    total = lax.psum(partial_value, "layer")
    half = partial_value.shape[1] // lax.axis_size("layer")
    first = lax.dynamic_slice_in_dim(total, lax.axis_index("layer") * half, half, 1).astype(jnp.bfloat16)
    second = multiply(first, right)
    return lax.psum_scatter(second, "layer", scatter_dimension=1, tiled=True).astype(jnp.bfloat16)


def product_kernel(flags, *refs, counts, start):
    count, pieces = counts
    near, far, own = refs[:count], refs[count : 2 * count], refs[2 * count]
    got, mate = refs[2 * count + 1 : 2 * count + 1 + pieces], refs[2 * count + 1 + pieces : 2 * count + 1 + 2 * pieces]
    kept, sent, lhs, rhs, total, lhs_sems, rhs_sems = refs[2 * count + 1 + 2 * pieces :]
    rows = kept.shape[1]
    depth, n = rhs.shape[1:]

    def half_of(operands, h):
        width = operands[0].shape[1]
        return operands[h * depth // width].at[:, pl.ds(h * depth % width, depth)]

    def lhs_copy(operands, h, chunk):
        return pltpu.make_async_copy(half_of(operands, h), lhs.at[chunk], lhs_sems.at[chunk])

    def rhs_copies(chunk):
        if chunk < 2:
            source = own.at[pl.ds(chunk * depth, depth), pl.ds(start, n)]
            return [pltpu.make_async_copy(source, rhs.at[chunk], rhs_sems.at[chunk, 0])]
        step = depth // pieces
        return [
            pltpu.make_async_copy(v, rhs.at[chunk, pl.ds(i * step, step)], rhs_sems.at[chunk, i])
            for i, v in enumerate(got if chunk == 2 else mate)
        ]

    for chunk in range(4):
        for own_near in (False, True):
            for upper in (False, True):
                if chunk < 2 and upper:
                    continue
                fits = flags[0] == int(own_near)
                if chunk >= 2:
                    fits &= flags[1] == int(upper)

                @pl.when(fits)
                def _():
                    operands = near if own_near == (chunk < 2) else far
                    h = chunk if chunk < 2 else int(upper) ^ (chunk - 2)
                    lhs_copy(operands, h, chunk).start()

        for copy in rhs_copies(chunk):
            copy.start()
    for chunk in range(4):
        lhs_copy(near, 0, chunk).wait()
        for copy in rhs_copies(chunk):
            copy.wait()
        term = jnp.dot(lhs[chunk], rhs[chunk], preferred_element_type=jnp.float32)
        if chunk == 0:
            total[...] = term
        elif chunk < 3:
            total[...] += term
        else:
            value = (total[...] + term).astype(kept.dtype)
            for i in range(4):
                (sent if i % 2 else kept)[i // 2] = value[i * rows : (i + 1) * rows]


def paired_rows(left, middle, right):
    rows, cols, layers = (lax.axis_size(a) for a in AXES)
    r, c, l = (lax.axis_index(a) for a in AXES)
    side, x, core = r >> 1, c >> 1, c & 1

    def send(v, to):
        pairs = []
        for i in range(rows):
            for j in range(cols):
                for k in range(layers):
                    t = to(i, j, k)
                    if t is None:
                        continue
                    pairs.append(((i * cols + j) * layers + k, (t[0] * cols + t[1]) * layers + t[2]))
        return lax.ppermute(v, AXES, pairs)

    beside = lambda v: send(v, lambda i, j, k: (i ^ 1, j, k))
    across = lambda v: send(v, lambda i, j, k: (i ^ 3, j, k))
    over_x = lambda v: send(v, lambda i, j, k: (i, j ^ 2, k))
    over_core = lambda v: send(v, lambda i, j, k: (i, j ^ 1, k))
    over_layer = lambda v: send(v, lambda i, j, k: (i, j, 1 - k))

    straight = x == side
    own_first = core == (r & 1)
    f32 = lambda v: v.astype(jnp.float32)
    bf16 = lambda v: v.astype(jnp.bfloat16)

    def in_order(flag, a, b, axis):
        return jnp.where(flag, jnp.concatenate([a, b], axis), jnp.concatenate([b, a], axis))

    def cut(w, start, size, pieces):
        part = w.shape[0] // layers
        step = part // pieces
        return [lax.dynamic_slice(w, (l * part + i * step, start), (step, size)) for i in range(pieces)]

    def fetch(pieces):
        got = [beside(v) for v in pieces]
        return got, [over_layer(v) for v in got]

    flags = jnp.stack([own_first, l == 1]).astype(jnp.int32)

    def times(near, far, own, start, fetched, after):
        got, mate = fetched
        *operands, _ = lax.optimization_barrier((*near, *far, *got, *mate, after[0]))
        operands.insert(2 * len(near), own)
        m, n, inner = near[0].shape[0], got[0].shape[1], 2 * own.shape[0]
        return pl.pallas_call(
            functools.partial(product_kernel, counts=(len(near), len(got)), start=start),
            in_specs=[pl.BlockSpec(memory_space=pltpu.SMEM)] + [pl.BlockSpec(memory_space=pl.ANY)] * len(operands),
            out_shape=[jax.ShapeDtypeStruct((2, m // 4, n), jnp.bfloat16)] * 2,
            scratch_shapes=[
                pltpu.VMEM((4, m, inner // 4), jnp.bfloat16),
                pltpu.VMEM((4, inner // 4, n), jnp.bfloat16),
                pltpu.VMEM((m, n), jnp.float32),
                pltpu.SemaphoreType.DMA((4,)),
                pltpu.SemaphoreType.DMA((4, len(got))),
            ],
            cost_estimate=pl.CostEstimate(
                flops=2 * m * n * inner, bytes_accessed=2 * (m * n + inner * (m + n)), transcendentals=0
            ),
        )(flags, *operands)

    half = left.shape[0] // layers
    width = left.shape[1]
    b = half // PIECES
    n = middle.shape[1]
    s = n // STRIPS
    mine = lax.dynamic_slice_in_dim(left, l * half, half, 0)
    theirs = lax.dynamic_slice_in_dim(left, (1 - l) * half, half, 0)

    def operand(p, before):
        keep = mine[p * b : (p + 1) * b]
        got = over_layer(theirs[p * b : (p + 1) * b])
        block = in_order(l == 0, keep, got, 1)
        over = lambda v, flag: send(v, lambda i, j, k: (i, j ^ 2, k) if (i >> 1 == j >> 1) == flag else None)
        upper = over(block[b // 2 :], False)
        stay = jnp.where(straight, block, over(block, True))
        go = jnp.where(straight, upper, block[: b // 2])
        got = across(go)
        a = jnp.concatenate([stay, in_order(straight, got, over_x(got), 0)], axis=0)
        a, *before = lax.optimization_barrier((a, *before))
        return (a, over_core(a)), before

    def reduce_first(part):
        mine, yours = part
        other = over_x(yours)
        stay, go = jnp.where(straight, mine, other), jnp.where(straight, other, mine)
        got = across(go)
        done = bf16(f32(stay) + f32(got[::-1]))
        a = jnp.stack([done, over_x(done)]).reshape(2 * b, s)
        return a, over_core(a)

    def reduce_second(part, i):
        mine, yours = part
        got = across(yours)
        final = lax.optimization_barrier(bf16(f32(mine) + f32(got[::-1])))
        return final, send(final, lambda a, j, k: None if k == i else (a, j, i))

    fetched = [fetch(cut(middle, i * s, s, FETCHES[f"m{i}"])) for i in range(STRIPS)]
    cuts = [cut(right, i * width, width, FETCHES[f"r{i}"]) for i in range(layers)]
    operands = [None] * PIECES
    for p in range(PIECES):
        operands[p], cuts[p] = operand(p, cuts[p])
    fetched_finals = [fetch(v) for v in cuts]
    parts, last = {}, (left,)
    for i in range(STRIPS):
        for p in range(PIECES):
            near, far = operands[p]
            parts[p, i] = last = times([near], [far], middle, i * s, fetched[i], last)
    firsts = {}
    for p in range(PIECES):
        firsts[p] = list(zip(*(reduce_first(parts[p, i]) for i in range(STRIPS))))
    kept, given = {}, {}
    for i in range(layers):
        for p in range(PIECES):
            last = times(*firsts[p], right, i * width, fetched_finals[i], last)
            kept[p, i], given[p, i] = reduce_second(last, i)
    results = [[jnp.where(l == 0, v[p, 0], v[p, 1]) for v in (kept, given)] for p in range(PIECES)]
    order = lambda v: jnp.where(straight, v, v[::-1]).reshape(b, width)
    own = jnp.concatenate([order(k) for k, _ in results], axis=0)
    other = jnp.concatenate([order(g) for _, g in results], axis=0)
    return in_order(l == 0, own, other, 0)


def solution(mesh):
    shape = mesh.shape
    fits = shape["row"] == shape["col"] == 4 and shape["layer"] == 2
    return jax.shard_map(
        paired_rows if fits else general,
        mesh=mesh,
        in_specs=(P("row", ("col", "layer")), P("row", "col"), P("row", "col")),
        out_specs=P("row", ("col", "layer")),
        check_vma=False,
    )
```

```python
import functools

import jax
import jax.numpy as jnp
from jax import lax
from jax.experimental import pallas as pl
from jax.experimental.pallas import tpu as pltpu
from jax.sharding import PartitionSpec as P


AXES = ("row", "col", "layer")
PIECES = 2
STRIPS = 2
SHARES = 2
FETCHES = {"m0": 2, "m1": 2, "r0": 1, "r1": 1, "r2": 1, "r3": 2}


def general(left, middle, right):
    def multiply(a, b):
        width = a.shape[1]
        layers = lax.axis_size("layer")
        groups = b.shape[0] // width // layers
        shaped = b.reshape(groups, layers, width, b.shape[1])
        own = lax.dynamic_index_in_dim(shaped, lax.axis_index("layer"), 1, keepdims=False)
        rows = lax.all_gather(own.reshape(groups * width, b.shape[1]), "row", axis=0, tiled=True)
        return jnp.dot(lax.all_gather(a, "col", axis=1, tiled=True), rows, preferred_element_type=jnp.float32)

    partial_value = multiply(left, middle)
    total = lax.psum(partial_value, "layer")
    half = partial_value.shape[1] // lax.axis_size("layer")
    first = lax.dynamic_slice_in_dim(total, lax.axis_index("layer") * half, half, 1).astype(jnp.bfloat16)
    second = multiply(first, right)
    return lax.psum_scatter(second, "layer", scatter_dimension=1, tiled=True).astype(jnp.bfloat16)


def product_kernel(flags, *refs, counts, start):
    groups, count, pieces = counts
    at = 2 * groups * count
    near = [refs[g * count : (g + 1) * count] for g in range(groups)]
    far = [refs[(groups + g) * count : (groups + g + 1) * count] for g in range(groups)]
    own, got, mate = refs[at], refs[at + 1 : at + 1 + pieces], refs[at + 1 + pieces : at + 1 + 2 * pieces]
    kept, sent, lhs, rhs, total, lhs_sems, rhs_sems = refs[at + 1 + 2 * pieces :]
    depth, n = rhs.shape[1:]
    block = kept.shape[2]
    m = 4 * block

    def lhs_copy(operands, h, chunk, g):
        width = operands[g][0].shape[1]
        source = operands[g][h * depth // width].at[:, pl.ds(h * depth % width, depth)]
        return pltpu.make_async_copy(source, lhs.at[chunk, pl.ds(g * m, m)], lhs_sems.at[chunk, g])

    def rhs_copies(chunk):
        if chunk < 2:
            source = own.at[pl.ds(chunk * depth, depth), pl.ds(start, n)]
            return [pltpu.make_async_copy(source, rhs.at[chunk], rhs_sems.at[chunk, 0])]
        step = depth // pieces
        return [
            pltpu.make_async_copy(v, rhs.at[chunk, pl.ds(i * step, step)], rhs_sems.at[chunk, i])
            for i, v in enumerate(got if chunk == 2 else mate)
        ]

    for chunk in range(4):
        for own_near in (False, True):
            for upper in (False, True):
                if chunk < 2 and upper:
                    continue
                fits = flags[0] == int(own_near)
                if chunk >= 2:
                    fits &= flags[1] == int(upper)

                @pl.when(fits)
                def _():
                    operands = near if own_near == (chunk < 2) else far
                    h = chunk if chunk < 2 else int(upper) ^ (chunk - 2)
                    for g in range(groups):
                        lhs_copy(operands, h, chunk, g).start()

        for copy in rhs_copies(chunk):
            copy.start()
    for chunk in range(4):
        for g in range(groups):
            lhs_copy(near, 0, chunk, g).wait()
        for copy in rhs_copies(chunk):
            copy.wait()

        def group(i, carry):
            rows = pl.ds(pl.multiple_of(i * m, m), m)
            term = jnp.dot(lhs[chunk, rows], rhs[chunk], preferred_element_type=jnp.float32)
            if chunk == 0:
                total[rows] = term
            elif chunk < 3:
                total[rows] += term
            else:
                value = (total[rows] + term).astype(kept.dtype)
                for j in range(4):
                    (sent if j % 2 else kept)[i, j // 2] = value[j * block : (j + 1) * block]
            return carry

        lax.fori_loop(0, groups, group, 0)


def paired_rows(left, middle, right):
    rows, cols, layers = (lax.axis_size(a) for a in AXES)
    r, c, l = (lax.axis_index(a) for a in AXES)
    side, x, core = r >> 1, c >> 1, c & 1

    def send(v, to):
        pairs = []
        for i in range(rows):
            for j in range(cols):
                for k in range(layers):
                    t = to(i, j, k)
                    if t is None:
                        continue
                    pairs.append(((i * cols + j) * layers + k, (t[0] * cols + t[1]) * layers + t[2]))
        return lax.ppermute(v, AXES, pairs)

    beside = lambda v: send(v, lambda i, j, k: (i ^ 1, j, k))
    across = lambda v: send(v, lambda i, j, k: (i ^ 3, j, k))
    over_x = lambda v: send(v, lambda i, j, k: (i, j ^ 2, k))
    over_core = lambda v: send(v, lambda i, j, k: (i, j ^ 1, k))
    over_layer = lambda v: send(v, lambda i, j, k: (i, j, 1 - k))

    straight = x == side
    own_first = core == (r & 1)
    f32 = lambda v: v.astype(jnp.float32)
    bf16 = lambda v: v.astype(jnp.bfloat16)

    def in_order(flag, a, b, axis):
        return jnp.where(flag, jnp.concatenate([a, b], axis), jnp.concatenate([b, a], axis))

    def cut(w, start, size, pieces):
        part = w.shape[0] // layers
        step = part // pieces
        return [lax.dynamic_slice(w, (l * part + i * step, start), (step, size)) for i in range(pieces)]

    def fetch(pieces):
        got = [beside(v) for v in pieces]
        return got, [over_layer(v) for v in got]

    flags = jnp.stack([own_first, l == 1]).astype(jnp.int32)

    def times(near, far, own, start, fetched, after):
        got, mate = fetched
        groups, count = len(near), len(near[0])
        near, far = [v for g in near for v in g], [v for g in far for v in g]
        *operands, _ = lax.optimization_barrier((*near, *far, *got, *mate, after[0]))
        operands.insert(len(near) + len(far), own)
        m, n, inner = near[0].shape[0], got[0].shape[1], 2 * own.shape[0]
        return pl.pallas_call(
            functools.partial(product_kernel, counts=(groups, count, len(got)), start=start),
            in_specs=[pl.BlockSpec(memory_space=pltpu.SMEM)] + [pl.BlockSpec(memory_space=pl.ANY)] * len(operands),
            out_shape=[jax.ShapeDtypeStruct((groups, 2, m // 4, n), jnp.bfloat16)] * 2,
            scratch_shapes=[
                pltpu.VMEM((4, groups * m, inner // 4), jnp.bfloat16),
                pltpu.VMEM((4, inner // 4, n), jnp.bfloat16),
                pltpu.VMEM((groups * m, n), jnp.float32),
                pltpu.SemaphoreType.DMA((4, groups)),
                pltpu.SemaphoreType.DMA((4, len(got))),
            ],
            cost_estimate=pl.CostEstimate(
                flops=2 * groups * m * n * inner,
                bytes_accessed=2 * (groups * m * (n + inner) + inner * n),
                transcendentals=0,
            ),
        )(flags, *operands)

    half = left.shape[0] // layers
    width = left.shape[1]
    b = half // PIECES
    n = middle.shape[1]
    s = n // STRIPS
    mine = lax.dynamic_slice_in_dim(left, l * half, half, 0)
    theirs = lax.dynamic_slice_in_dim(left, (1 - l) * half, half, 0)

    def operand(p, before):
        keep = mine[p * b : (p + 1) * b]
        got = over_layer(theirs[p * b : (p + 1) * b])
        block = in_order(l == 0, keep, got, 1)
        over = lambda v, flag: send(v, lambda i, j, k: (i, j ^ 2, k) if (i >> 1 == j >> 1) == flag else None)
        upper = over(block[b // 2 :], False)
        stay = jnp.where(straight, block, over(block, True))
        go = jnp.where(straight, upper, block[: b // 2])
        got = across(go)
        a = jnp.concatenate([stay, in_order(straight, got, over_x(got), 0)], axis=0)
        a, *before = lax.optimization_barrier((a, *before))
        return (a, over_core(a)), before

    def reduce_first(part):
        mine, yours = part[0][0], part[1][0]
        other = over_x(yours)
        stay, go = jnp.where(straight, mine, other), jnp.where(straight, other, mine)
        got = across(go)
        done = bf16(f32(stay) + f32(got[::-1]))
        a = jnp.stack([done, over_x(done)]).reshape(2 * b, s)
        return a, over_core(a)

    def reduce_second(part, owner):
        mine, yours = part
        got = across(yours)
        final = lax.optimization_barrier(bf16(f32(mine) + f32(got[:, ::-1])))
        return final, send(final, lambda i, j, k: None if k == owner else (i, j, owner))

    fetched = [fetch(cut(middle, i * s, s, FETCHES[f"m{i}"])) for i in range(STRIPS)]
    share = width // SHARES
    cuts = [cut(right, i * share, share, FETCHES[f"r{i}"]) for i in range(layers * SHARES)]
    operands = [None] * PIECES

    def regroup(pair, flat, like):
        flat = iter(flat)
        return pair, [[next(flat) for _ in v] for v in like]

    for p in range(PIECES):
        operands[p], cuts[p::PIECES] = regroup(*operand(p, [v for c in cuts[p::PIECES] for v in c]), cuts[p::PIECES])
    fetched_finals = [fetch(v) for v in cuts]
    parts, last = {}, (left,)
    for i in range(STRIPS):
        for p in range(PIECES):
            near, far = operands[p]
            parts[p, i] = last = times([[near]], [[far]], middle, i * s, fetched[i], last)
    firsts = {}
    for p in range(PIECES):
        firsts[p] = list(zip(*(reduce_first(parts[p, i]) for i in range(STRIPS))))
    kept, given = {}, {}
    for i in range(layers * SHARES):
        alone = [[p] for p in range(PIECES)] if i == 0 else [list(range(PIECES))]
        for members in alone:
            near, far = zip(*(firsts[p] for p in members))
            last = times(near, far, right, i * share, fetched_finals[i], last)
            final, moved = reduce_second(last, i // SHARES)
            for at, p in enumerate(members):
                kept[p, i], given[p, i] = final[at], moved[at]

    def collect(v, p):
        parts = [[v[p, owner * SHARES + i] for i in range(SHARES)] for owner in range(layers)]
        return jnp.where(l == 0, *(jnp.concatenate(t, axis=2) for t in parts))

    results = [[collect(v, p) for v in (kept, given)] for p in range(PIECES)]
    order = lambda v: jnp.where(straight, v, v[::-1]).reshape(b, width)
    own = jnp.concatenate([order(k) for k, _ in results], axis=0)
    other = jnp.concatenate([order(g) for _, g in results], axis=0)
    return in_order(l == 0, own, other, 0)


def solution(mesh):
    shape = mesh.shape
    fits = shape["row"] == shape["col"] == 4 and shape["layer"] == 2
    return jax.shard_map(
        paired_rows if fits else general,
        mesh=mesh,
        in_specs=(P("row", ("col", "layer")), P("row", "col"), P("row", "col")),
        out_specs=P("row", ("col", "layer")),
        check_vma=False,
    )
```

```python
import functools

import jax
import jax.numpy as jnp
from jax import lax
from jax.experimental import pallas as pl
from jax.experimental.pallas import tpu as pltpu
from jax.sharding import PartitionSpec as P


AXES = ("row", "col", "layer")
PIECES = 2
STRIPS = 2
SHARES = 2
FETCHES = {"m0": 2, "m1": 2, "r0": 1, "r1": 1, "r2": 1, "r3": 2}


def general(left, middle, right):
    def multiply(a, b):
        width = a.shape[1]
        layers = lax.axis_size("layer")
        groups = b.shape[0] // width // layers
        shaped = b.reshape(groups, layers, width, b.shape[1])
        own = lax.dynamic_index_in_dim(shaped, lax.axis_index("layer"), 1, keepdims=False)
        rows = lax.all_gather(own.reshape(groups * width, b.shape[1]), "row", axis=0, tiled=True)
        return jnp.dot(lax.all_gather(a, "col", axis=1, tiled=True), rows, preferred_element_type=jnp.float32)

    partial_value = multiply(left, middle)
    total = lax.psum(partial_value, "layer")
    half = partial_value.shape[1] // lax.axis_size("layer")
    first = lax.dynamic_slice_in_dim(total, lax.axis_index("layer") * half, half, 1).astype(jnp.bfloat16)
    second = multiply(first, right)
    return lax.psum_scatter(second, "layer", scatter_dimension=1, tiled=True).astype(jnp.bfloat16)


def product_kernel(flags, *refs, counts, start):
    groups, count, pieces = counts
    at = 2 * groups * count
    near = [refs[g * count : (g + 1) * count] for g in range(groups)]
    far = [refs[(groups + g) * count : (groups + g + 1) * count] for g in range(groups)]
    own, got, mate = refs[at], refs[at + 1 : at + 1 + pieces], refs[at + 1 + pieces : at + 1 + 2 * pieces]
    kept, sent, lhs, rhs, total, lhs_sems, rhs_sems = refs[at + 1 + 2 * pieces :]
    depth, n = rhs.shape[1:]
    block = kept.shape[2]
    m = 4 * block

    def lhs_copy(operands, h, chunk, g):
        width = operands[g][0].shape[1]
        source = operands[g][h * depth // width].at[:, pl.ds(h * depth % width, depth)]
        return pltpu.make_async_copy(source, lhs.at[chunk, pl.ds(g * m, m)], lhs_sems.at[chunk, g])

    def rhs_copies(chunk):
        if chunk < 2:
            source = own.at[pl.ds(chunk * depth, depth), pl.ds(start, n)]
            return [pltpu.make_async_copy(source, rhs.at[chunk], rhs_sems.at[chunk, 0])]
        step = depth // pieces
        return [
            pltpu.make_async_copy(v, rhs.at[chunk, pl.ds(i * step, step)], rhs_sems.at[chunk, i])
            for i, v in enumerate(got if chunk == 2 else mate)
        ]

    for chunk in range(4):
        for own_near in (False, True):
            for upper in (False, True):
                if chunk < 2 and upper:
                    continue
                fits = flags[0] == int(own_near)
                if chunk >= 2:
                    fits &= flags[1] == int(upper)

                @pl.when(fits)
                def _():
                    operands = near if own_near == (chunk < 2) else far
                    h = chunk if chunk < 2 else int(upper) ^ (chunk - 2)
                    for g in range(groups):
                        lhs_copy(operands, h, chunk, g).start()

        for copy in rhs_copies(chunk):
            copy.start()
    for chunk in range(4):
        for g in range(groups):
            lhs_copy(near, 0, chunk, g).wait()
        for copy in rhs_copies(chunk):
            copy.wait()

        def group(i, carry):
            rows = pl.ds(pl.multiple_of(i * m, m), m)
            term = jnp.dot(lhs[chunk, rows], rhs[chunk], preferred_element_type=jnp.float32)
            if chunk == 0:
                total[rows] = term
            elif chunk < 3:
                total[rows] += term
            else:
                value = (total[rows] + term).astype(kept.dtype)
                for j in range(4):
                    (sent if j % 2 else kept)[i, j // 2] = value[j * block : (j + 1) * block]
            return carry

        lax.fori_loop(0, groups, group, 0)


def paired_rows(left, middle, right):
    rows, cols, layers = (lax.axis_size(a) for a in AXES)
    r, c, l = (lax.axis_index(a) for a in AXES)
    side, x, core = r >> 1, c >> 1, c & 1

    def send(v, to):
        pairs = []
        for i in range(rows):
            for j in range(cols):
                for k in range(layers):
                    t = to(i, j, k)
                    if t is None:
                        continue
                    pairs.append(((i * cols + j) * layers + k, (t[0] * cols + t[1]) * layers + t[2]))
        return lax.ppermute(v, AXES, pairs)

    beside = lambda v: send(v, lambda i, j, k: (i ^ 1, j, k))
    across = lambda v: send(v, lambda i, j, k: (i ^ 3, j, k))
    over_x = lambda v: send(v, lambda i, j, k: (i, j ^ 2, k))
    over_core = lambda v: send(v, lambda i, j, k: (i, j ^ 1, k))
    over_layer = lambda v: send(v, lambda i, j, k: (i, j, 1 - k))

    straight = x == side
    own_first = core == (r & 1)
    f32 = lambda v: v.astype(jnp.float32)
    bf16 = lambda v: v.astype(jnp.bfloat16)

    def in_order(flag, a, b, axis):
        return jnp.where(flag, jnp.concatenate([a, b], axis), jnp.concatenate([b, a], axis))

    def cut(w, start, size, pieces):
        part = w.shape[0] // layers
        step = part // pieces
        return [lax.dynamic_slice(w, (l * part + i * step, start), (step, size)) for i in range(pieces)]

    def fetch(pieces):
        got = [beside(v) for v in pieces]
        return got, [over_layer(v) for v in got]

    flags = jnp.stack([own_first, l == 1]).astype(jnp.int32)

    def times(near, far, own, start, fetched, after):
        got, mate = fetched
        groups, count = len(near), len(near[0])
        near, far = [v for g in near for v in g], [v for g in far for v in g]
        *operands, _ = lax.optimization_barrier((*near, *far, *got, *mate, after[0]))
        operands.insert(len(near) + len(far), own)
        m, n, inner = near[0].shape[0], got[0].shape[1], 2 * own.shape[0]
        return pl.pallas_call(
            functools.partial(product_kernel, counts=(groups, count, len(got)), start=start),
            in_specs=[pl.BlockSpec(memory_space=pltpu.SMEM)] + [pl.BlockSpec(memory_space=pl.ANY)] * len(operands),
            out_shape=[jax.ShapeDtypeStruct((groups, 2, m // 4, n), jnp.bfloat16)] * 2,
            scratch_shapes=[
                pltpu.VMEM((4, groups * m, inner // 4), jnp.bfloat16),
                pltpu.VMEM((4, inner // 4, n), jnp.bfloat16),
                pltpu.VMEM((groups * m, n), jnp.float32),
                pltpu.SemaphoreType.DMA((4, groups)),
                pltpu.SemaphoreType.DMA((4, len(got))),
            ],
            cost_estimate=pl.CostEstimate(
                flops=2 * groups * m * n * inner,
                bytes_accessed=2 * (groups * m * (n + inner) + inner * n),
                transcendentals=0,
            ),
        )(flags, *operands)

    half = left.shape[0] // layers
    width = left.shape[1]
    b = half // PIECES
    n = middle.shape[1]
    s = n // STRIPS
    mine = lax.dynamic_slice_in_dim(left, l * half, half, 0)
    theirs = lax.dynamic_slice_in_dim(left, (1 - l) * half, half, 0)

    def operand(p, before):
        keep = mine[p * b : (p + 1) * b]
        got = over_layer(theirs[p * b : (p + 1) * b])
        block = in_order(l == 0, keep, got, 1)
        over = lambda v, flag: send(v, lambda i, j, k: (i, j ^ 2, k) if (i >> 1 == j >> 1) == flag else None)
        upper = over(block[b // 2 :], False)
        stay = jnp.where(straight, block, over(block, True))
        go = jnp.where(straight, upper, block[: b // 2])
        got = across(go)
        a = jnp.concatenate([stay, in_order(straight, got, over_x(got), 0)], axis=0)
        a, *before = lax.optimization_barrier((a, *before))
        return (a, over_core(a)), before

    def reduce_first(part):
        mine, yours = part[0][0], part[1][0]
        other = over_x(yours)
        stay, go = jnp.where(straight, mine, other), jnp.where(straight, other, mine)
        got = across(go)
        done = bf16(f32(stay) + f32(got[::-1]))
        a = jnp.stack([done, over_x(done)]).reshape(2 * b, s)
        return a, over_core(a)

    def reduce_second(part, owner):
        mine, yours = part
        got = across(yours)
        final = lax.optimization_barrier(bf16(f32(mine) + f32(got[:, ::-1])))
        return final, send(final, lambda i, j, k: None if k == owner else (i, j, owner))

    fetched = [fetch(cut(middle, i * s, s, FETCHES[f"m{i}"])) for i in range(STRIPS)]
    share = width // SHARES
    cuts = [cut(right, i * share, share, FETCHES[f"r{i}"]) for i in range(layers * SHARES)]
    operands = [None] * PIECES

    def regroup(pair, flat, like):
        flat = iter(flat)
        return pair, [[next(flat) for _ in v] for v in like]

    for p in range(PIECES):
        operands[p], cuts[p::PIECES] = regroup(*operand(p, [v for c in cuts[p::PIECES] for v in c]), cuts[p::PIECES])
    fetched_finals = [fetch(v) for v in cuts]
    parts, last = {}, (left,)
    for i in range(STRIPS):
        for p in range(PIECES):
            near, far = operands[p]
            parts[p, i] = last = times([[near]], [[far]], middle, i * s, fetched[i], last)
    firsts = {}
    for p in range(PIECES):
        firsts[p] = list(zip(*(reduce_first(parts[p, i]) for i in range(STRIPS))))
    kept, given = {}, {}
    jobs = [(i, [p]) for p in range(PIECES) for i in range(SHARES)]
    jobs += [(i, list(range(PIECES))) for i in range(SHARES, layers * SHARES)]
    for i, members in jobs:
        near, far = zip(*(firsts[p] for p in members))
        last = times(near, far, right, i * share, fetched_finals[i], last)
        final, moved = reduce_second(last, i // SHARES)
        for at, p in enumerate(members):
            kept[p, i], given[p, i] = final[at], moved[at]

    def collect(v, p):
        parts = [[v[p, owner * SHARES + i] for i in range(SHARES)] for owner in range(layers)]
        return jnp.where(l == 0, *(jnp.concatenate(t, axis=2) for t in parts))

    results = [[collect(v, p) for v in (kept, given)] for p in range(PIECES)]
    order = lambda v: jnp.where(straight, v, v[::-1]).reshape(b, width)
    own = jnp.concatenate([order(k) for k, _ in results], axis=0)
    other = jnp.concatenate([order(g) for _, g in results], axis=0)
    return in_order(l == 0, own, other, 0)


def solution(mesh):
    shape = mesh.shape
    fits = shape["row"] == shape["col"] == 4 and shape["layer"] == 2
    return jax.shard_map(
        paired_rows if fits else general,
        mesh=mesh,
        in_specs=(P("row", ("col", "layer")), P("row", "col"), P("row", "col")),
        out_specs=P("row", ("col", "layer")),
        check_vma=False,
    )
```
